32 devices in a mesh: shard: 16 (over z, y, core), model: 2 (over x).
Axes of the slice: x: 2, y: 2, z: 4, core: 2. Of those that a mesh axis runs over, the one named last changes fastest.
Arguments:
- gradients: float32 [128, 128, 4096], P(None, 'shard', 'model'), may hold values from -6 to 6
- momentum: float32 [128, 128, 4096], P(None, 'shard', 'model'), may hold values from -6 to 6
- weights: float32 [128, 128, 4096], P(None, 'shard', 'model'), may hold values from -0.1875 to 0.1875
Outputs:
- new_weights: float32 [128, 128, 4096], P(None, 'shard', 'model')
- new_momentum: float32 [128, 128, 4096], P(None, 'shard', 'model')
The draws below stay inside these ranges and needn't reach their ends.
All inputs are finite; a program needn't handle non-finite values.
Results may differ from the reference program's by a relative error of at most 0.0001.
Values sent between devices are 32-bit elements; how exact they have to be, the bound alone decides.
A program may use at most 128 MiB of HBM per device.

```python
import jax
import jax.numpy as jnp
from jax import lax

SIDE = 128
WIDE = 4096
MATS = 128
ITERS = 3


def steps_of(stream_key, shape, pieces, low, largest):
    loudness, own = 1.0, jax.random.fold_in(stream_key, 6)
    for dim, parts in pieces:
        steps = jnp.exp(jax.random.uniform(jax.random.fold_in(own, dim), (parts,), jnp.float32, low / len(pieces), largest / len(pieces)))
        loudness = loudness * jnp.repeat(steps, shape[dim] // parts).reshape([-1 if axis == dim else 1 for axis in range(len(shape))])
    return loudness


def scatter_about(rng, shape, spread, bound, split=(), kind=jnp.bfloat16):
    entries = spread * jax.random.normal(rng, shape, jnp.float32)
    if split:
        entries = entries * steps_of(rng, shape, split, -0.22, 0.18)
    return jnp.clip(entries, -bound, bound).astype(kind)


def setup_inputs(seed: int = 0) -> dict:
    key_of = jax.random.split(jax.random.key(seed), 4)
    gradients = scatter_about(key_of[0], (MATS, SIDE, WIDE), 1.0, 6.0, ((1, 16), (2, 2)), jnp.float32)
    momentum = scatter_about(key_of[1], (MATS, SIDE, WIDE), 1.0, 6.0, ((1, 16), (2, 2)), jnp.float32)
    weights = scatter_about(key_of[2], (MATS, SIDE, WIDE), 0.03, 0.1875, ((1, 16), (2, 2)), jnp.float32)
    return dict(gradients=gradients, momentum=momentum, weights=weights)


hold_rate = 0.9
learn_rate = 0.9
decay_rate = 0.1

def reference(gradients, momentum, weights):
    new_momentum = hold_rate * momentum + gradients

    def orthogonal_one(stack):
        iterate = stack[None]
        iterate = iterate * lax.rsqrt(lax.optimization_barrier(jnp.sum(iterate * iterate, axis=(1, 2), keepdims=True)) + 1e-06)
        for step in range(ITERS):
            gram = jnp.einsum('mik,mjk->mij', iterate, iterate, precision=lax.Precision.HIGHEST)
            mixed = -4.775 * gram + 2.0315 * jnp.einsum('mij,mjk->mik', gram, gram, precision=lax.Precision.HIGHEST)
            iterate = 3.4445 * iterate + jnp.einsum('mij,mjk->mik', mixed, iterate, precision=lax.Precision.HIGHEST)
        return iterate[0]
    iterate = lax.map(orthogonal_one, new_momentum)
    new_weights = (1.0 - learn_rate * decay_rate) * weights - learn_rate * iterate
    return (new_weights, new_momentum)
```

```python
import functools

import jax
import jax.numpy as jnp
from jax import lax
from jax.experimental import pallas as pl
from jax.experimental.pallas import tpu as pltpu
from jax.sharding import PartitionSpec as P

ITERS = 3
AHEAD = 2
BEHIND = 3

hold_rate = 0.9
learn_rate = 0.9
decay_rate = 0.1

MESH = pl.DeviceIdType.MESH


def dot(a, b, contract):
    return lax.dot_general(
        a,
        b,
        ((contract[0], contract[1]), ((), ())),
        precision=lax.Precision.HIGHEST,
        preferred_element_type=jnp.float32,
    )


def mul(a, b):
    return dot(a, b, ((1,), (0,)))


def mixer(gram, eye):
    total = jnp.sum(jnp.sum(gram * eye, axis=1, keepdims=True), axis=0, keepdims=True)
    scale = lax.rsqrt(total + 1e-06)
    a = gram * scale * scale
    q = None
    for step in range(ITERS):
        p = 3.4445 * eye + (-4.775 * a + 2.0315 * mul(a, a))
        q = p if q is None else mul(p, q)
        if step < ITERS - 1:
            a = mul(mul(p, a), p)
    return q * scale


def flipped(me, k, n):
    out, bit = 0, 1
    while bit < n:
        own = (me // bit) % 2
        out = out + bit * ((1 - own) if (k // bit) % 2 else own)
        bit *= 2
    return out


def partners(me, n):
    if n < 4:
        return [flipped(me, k, n) for k in range(1, n)]
    part = n // 4
    at, low = me // part, me % part
    upper = at // 2
    far, near, beside = 3 * (1 - upper), 2 - upper, at + 1 - 2 * (at % 2)
    lows = [flipped(low, k, part) for k in range(part)]
    across = [part * at + k for at in (far, near) for k in lows]
    within = [part * beside + k for k in lows] + [part * at + k for k in lows[1:]]
    order = [None] * (n - 1)
    order[0::2], order[1::2] = across, within
    return order


def step_kernel(
    n, models, grad_ref, mom_ref, weight_ref, out_ref, new_ref, wlast_ref,
    x, gs, ms, ws, gram, peers, gload, mload, wload, lload, send1, recv1, send2, recv2, gsend, grecv,
):
    me = lax.axis_index("shard")
    col = lax.axis_index("model")
    _, per, rows, cols = grad_ref.shape
    side = n * rows
    chunk = min(cols, 512)
    dests = partners(me, n)
    mine = pl.ds(pl.multiple_of(me * rows, rows), rows)

    def loads(c):
        slot = c % 2
        return (
            pltpu.make_async_copy(grad_ref.at[:, c], gs.at[slot], gload.at[slot]),
            pltpu.make_async_copy(mom_ref.at[:, c], ms.at[slot], mload.at[slot]),
        )

    def weight_load(c):
        slot = c % 2
        return pltpu.make_async_copy(weight_ref.at[:, c], ws.at[slot], wload.at[slot])

    def last_load():
        return pltpu.make_async_copy(weight_ref.at[:, per - 1], wlast_ref, lload)

    def load(c):
        for copy in loads(c):
            copy.start()

    def make(c):
        for copy in loads(c):
            copy.wait()
        slot = c % 2

        def one(j, carry):
            new_ref[j, c] = hold_rate * ms[slot, j] + gs[slot, j]
            return carry

        lax.fori_loop(0, n, one, 0)

    def finish(c):
        got = out_ref.at[:, c]
        pltpu.make_async_copy(got, got, recv2.at[c]).wait()
        weight_load(c).wait()
        slot = c % 2

        def one(j, carry):
            out_ref[j, c] = (1.0 - learn_rate * decay_rate) * ws[slot, j] - learn_rate * out_ref[j, c]
            return carry

        lax.fori_loop(0, n, one, 0)

    def forth(c):
        for dest in dests:
            pltpu.make_async_remote_copy(
                src_ref=new_ref.at[dest, c],
                dst_ref=x.at[c, mine, :],
                send_sem=send1.at[c],
                recv_sem=recv1.at[c],
                device_id={"shard": dest},
                device_id_type=MESH,
            ).start()
        pltpu.make_async_copy(new_ref.at[me, c], x.at[c, mine, :], recv1.at[c]).start()

    def back(c):
        for dest in dests:
            theirs = pl.ds(pl.multiple_of(dest * rows, rows), rows)
            pltpu.make_async_remote_copy(
                src_ref=x.at[c, theirs, :],
                dst_ref=out_ref.at[me, c],
                send_sem=send2.at[c],
                recv_sem=recv2.at[c],
                device_id={"shard": dest},
                device_id_type=MESH,
            ).start()
        pltpu.make_async_copy(x.at[c, mine, :], out_ref.at[me, c], recv2.at[c]).start()

    barrier = pltpu.get_barrier_semaphore()
    for dest in dests:
        pl.semaphore_signal(barrier, inc=1, device_id={"shard": dest}, device_id_type=MESH)
    for step in range(1, models):
        pl.semaphore_signal(barrier, inc=1, device_id={"model": (col + step) % models}, device_id_type=MESH)
    for c in range(min(2, per)):
        load(c)
        weight_load(c).start()
    make(0)
    pl.semaphore_wait(barrier, n - 1 + models - 1)
    forth(0)
    for c in range(2, min(AHEAD + 2, per + 1)):
        if c < per:
            load(c)
        make(c - 1)
    for c in range(1, min(AHEAD, per)):
        forth(c)
    last_load().start()

    eye = (
        lax.broadcasted_iota(jnp.int32, (side, side), 0) == lax.broadcasted_iota(jnp.int32, (side, side), 1)
    ).astype(jnp.float32)

    def round_(c, carry):
        pltpu.make_async_copy(x.at[c], x.at[c], recv1.at[c]).wait()

        def part(k, total):
            piece = x[c, :, pl.ds(pl.multiple_of(k * chunk, chunk), chunk)]
            return total + dot(piece, piece, ((1,), (1,)))

        gram[c] = lax.fori_loop(0, cols // chunk, part, jnp.zeros((side, side), jnp.float32))

        @pl.when(c + AHEAD < per)
        def _():
            forth(c + AHEAD)

        copies = []
        for step in range(1, models):
            copy = pltpu.make_async_remote_copy(
                src_ref=gram.at[c],
                dst_ref=peers.at[step - 1, c],
                send_sem=gsend.at[step - 1, c],
                recv_sem=grecv.at[step - 1, c],
                device_id={"model": (col + step) % models},
                device_id_type=MESH,
            )
            copy.start()
            copies.append(copy)
        whole = gram[c]
        for step, copy in enumerate(copies):
            copy.wait()
            whole = whole + peers[step, c]
        q = mixer(whole, eye)

        def apply(k, carry):
            at = pl.ds(pl.multiple_of(k * chunk, chunk), chunk)
            x[c, :, at] = mul(q, x[c, :, at])
            return carry

        lax.fori_loop(0, cols // chunk, apply, 0)

        @pl.when(c + AHEAD + 1 < per)
        def _():
            make(c + AHEAD + 1)

        @pl.when(c + AHEAD + 2 < per)
        def _():
            load(c + AHEAD + 2)

        back(c)

        @pl.when(c >= BEHIND)
        def _():
            finish(c - BEHIND)

            @pl.when(c - BEHIND + 2 < per - 1)
            def _():
                weight_load(c - BEHIND + 2).start()

        return carry

    lax.fori_loop(0, per, round_, 0)

    def drain(c, carry):
        sent = x.at[c, pl.ds(0, side - rows), :]
        pltpu.make_async_copy(sent, sent, send1.at[c]).wait()
        return carry

    lax.fori_loop(0, per, drain, 0)

    def last(c, carry):
        finish(c)

        @pl.when(c + 2 < per - 1)
        def _():
            weight_load(c + 2).start()

        return carry

    lax.fori_loop(max(per - BEHIND, 0), per - 1, last, 0)
    got = out_ref.at[:, per - 1]
    pltpu.make_async_copy(got, got, recv2.at[per - 1]).wait()
    last_load().wait()

    def drain_back(c, carry):
        sent = x.at[c, pl.ds(0, side - rows), :]
        pltpu.make_async_copy(sent, sent, send2.at[c]).wait()
        return carry

    lax.fori_loop(0, per, drain_back, 0)


def close_kernel(out_ref, new_ref, wlast_ref, weights_ref, momentum_ref, stage, sems):
    n, per, _, _ = out_ref.shape
    pieces = 4
    copies = []
    for k in range(pieces):
        at = pl.ds(k * (n // pieces), n // pieces)
        copies.append((new_ref.at[at], momentum_ref.at[at]))
        early = pl.ds(0, per - 1)
        copies.append((out_ref.at[at, early], weights_ref.at[at, early]))
    copies = [pltpu.make_async_copy(src, dst, sems.at[k]) for k, (src, dst) in enumerate(copies)]
    for copy in copies:
        copy.start()

    def one(j, carry):
        stage[j] = (1.0 - learn_rate * decay_rate) * wlast_ref[j] - learn_rate * out_ref[j, per - 1]
        return carry

    lax.fori_loop(0, n, one, 0)
    end = pltpu.make_async_copy(stage, weights_ref.at[:, per - 1], sems.at[2 * pieces])
    end.start()
    for copy in copies:
        copy.wait()
    end.wait()


def step_direct(gradients, momentum, weights, n, models):
    mats, rows, cols = gradients.shape
    per, side = mats // n, n * rows
    others = max(models - 1, 1)
    split = (n, per, rows, cols)
    placed = pltpu.VMEM(split, jnp.float32)
    slab = pltpu.VMEM((n, rows, cols), jnp.float32)
    held = pl.pallas_call(
        functools.partial(step_kernel, n, models),
        out_shape=(placed, placed, slab),
        in_specs=[pl.BlockSpec(memory_space=pltpu.HBM)] * 3,
        out_specs=[pl.BlockSpec(memory_space=pltpu.VMEM)] * 3,
        scratch_shapes=[
            pltpu.VMEM((per, side, cols), jnp.float32),
            pltpu.VMEM((2, n, rows, cols), jnp.float32),
            pltpu.VMEM((2, n, rows, cols), jnp.float32),
            pltpu.VMEM((2, n, rows, cols), jnp.float32),
            pltpu.VMEM((per, side, side), jnp.float32),
            pltpu.VMEM((others, per, side, side), jnp.float32),
            pltpu.SemaphoreType.DMA((2,)),
            pltpu.SemaphoreType.DMA((2,)),
            pltpu.SemaphoreType.DMA((2,)),
            pltpu.SemaphoreType.DMA,
            pltpu.SemaphoreType.DMA((per,)),
            pltpu.SemaphoreType.DMA((per,)),
            pltpu.SemaphoreType.DMA((per,)),
            pltpu.SemaphoreType.DMA((per,)),
            pltpu.SemaphoreType.DMA((others, per)),
            pltpu.SemaphoreType.DMA((others, per)),
        ],
        compiler_params=pltpu.CompilerParams(
            collective_id=0, has_side_effects=True, vmem_limit_bytes=40 * 1024 * 1024
        ),
    )(*(array.reshape(split) for array in (gradients, momentum, weights)))
    out, new = pl.pallas_call(
        close_kernel,
        out_shape=(jax.ShapeDtypeStruct(split, jnp.float32),) * 2,
        in_specs=[pl.BlockSpec(memory_space=pltpu.VMEM)] * 3,
        out_specs=[pl.BlockSpec(memory_space=pltpu.HBM)] * 2,
        scratch_shapes=[pltpu.VMEM((n, rows, cols), jnp.float32), pltpu.SemaphoreType.DMA((9,))],
        compiler_params=pltpu.CompilerParams(vmem_limit_bytes=4 * 1024 * 1024),
    )(*(pltpu.with_memory_space_constraint(array, pltpu.VMEM) for array in held))
    return out.reshape(gradients.shape), new.reshape(gradients.shape)


def exchange_plain(new_momentum):
    moved = lax.all_to_all(new_momentum, "shard", split_axis=0, concat_axis=1, tiled=True)
    gram = lax.psum(
        jnp.einsum("mik,mjk->mij", moved, moved, precision=lax.Precision.HIGHEST), "model"
    )
    eye = jnp.eye(gram.shape[-1], dtype=jnp.float32)
    q = jax.vmap(lambda g: mixer(g, eye))(gram)
    iterate = jnp.einsum("mij,mjk->mik", q, moved, precision=lax.Precision.HIGHEST)
    return lax.all_to_all(iterate, "shard", split_axis=1, concat_axis=0, tiled=True)


def body(n, models, gradients, momentum, weights):
    mats, rows, cols = gradients.shape
    size = mats * rows * cols * 4
    if n & (n - 1) == 0 and rows % 8 == 0 and cols % 128 == 0 and size <= 8 << 20 and mats // n > BEHIND and n % 4 == 0:
        return step_direct(gradients, momentum, weights, n, models)
    new_momentum = hold_rate * momentum + gradients
    back = exchange_plain(new_momentum)
    new_weights = (1.0 - learn_rate * decay_rate) * weights - learn_rate * back
    return (new_weights, new_momentum)


def solution(mesh):
    placed = (P(None, "shard", "model"), P(None, "shard", "model"), P(None, "shard", "model"))
    return jax.shard_map(
        functools.partial(body, mesh.shape["shard"], mesh.shape["model"]),
        mesh=mesh,
        in_specs=placed,
        out_specs=(P(None, "shard", "model"), P(None, "shard", "model")),
        check_vma=False,
    )
```

```python
import functools

import jax
import jax.numpy as jnp
from jax import lax
from jax.experimental import pallas as pl
from jax.experimental.pallas import tpu as pltpu
from jax.sharding import PartitionSpec as P

ITERS = 3
AHEAD = 4
LATE = 3
HELD = 1

hold_rate = 0.9
learn_rate = 0.9
decay_rate = 0.1

MESH = pl.DeviceIdType.MESH


def dot(a, b, contract):
    return lax.dot_general(
        a,
        b,
        ((contract[0], contract[1]), ((), ())),
        precision=lax.Precision.HIGHEST,
        preferred_element_type=jnp.float32,
    )


def mul(a, b):
    return dot(a, b, ((1,), (0,)))


def mixer(gram, eye):
    total = jnp.sum(jnp.sum(gram * eye, axis=1, keepdims=True), axis=0, keepdims=True)
    scale = lax.rsqrt(total + 1e-06)
    a = gram * scale * scale
    q = None
    for step in range(ITERS):
        p = 3.4445 * eye + (-4.775 * a + 2.0315 * mul(a, a))
        q = p if q is None else mul(p, q)
        if step < ITERS - 1:
            a = mul(mul(p, a), p)
    return q * scale


def flipped(me, k, n):
    out, bit = 0, 1
    while bit < n:
        own = (me // bit) % 2
        out = out + bit * ((1 - own) if (k // bit) % 2 else own)
        bit *= 2
    return out


def quarters(me, n):
    at = me // (n // 4)
    upper = at // 2
    return at, at + 1 - 2 * (at % 2), 2 - upper, 3 * (1 - upper)


def members(me, n, quarter):
    part = n // 4
    return [part * quarter + flipped(me % part, k, part) for k in range(part)]


def woven(first, second):
    order = []
    for k in range(max(len(first), len(second))):
        order += first[k : k + 1] + second[k : k + 1]
    return order


def partners(me, n):
    own, beside, near, far = (members(me, n, quarter) for quarter in quarters(me, n))
    return woven(far + near, beside + own[1:])


def signal(semaphore, dest):
    pl.semaphore_signal(semaphore, inc=1, device_id={"shard": dest}, device_id_type=MESH)


def greet(me, n, middle):
    _, beside, near, _ = quarters(me, n)
    barrier = pltpu.get_barrier_semaphore()

    @pl.when(middle)
    def _():
        for dest in members(me, n, near) + members(me, n, beside):
            signal(barrier, dest)

    own = members(me, n, quarters(me, n)[0])
    for dest in own[1:]:
        signal(barrier, dest)
    return barrier, len(own) * 2 - 1


def enter(me, n, middle, inside):
    @pl.when(jnp.logical_not(middle))
    def _():
        for dest in members(me, n, quarters(me, n)[1]):
            signal(inside, dest)


def pass_across(me, n, middle, inside, passed):
    @pl.when(middle)
    def _():
        pl.semaphore_wait(inside, n // 4)
        signal(passed, members(me, n, quarters(me, n)[2])[0])


def pass_outward(me, n, middle, passed):
    pl.semaphore_wait(passed, 1)

    @pl.when(middle)
    def _():
        signal(passed, members(me, n, quarters(me, n)[1])[0])


def step_kernel(
    n, models, grad_ref, mom_ref, weight_ref, out_ref, new_ref, x,
    gs, ms, ws, gram, peers, gload, mload, wload, qload, send1, recv1, send2, recv2, hsend, hrecv, gsend, grecv, inside, passed,
):
    me = lax.axis_index("shard")
    col = lax.axis_index("model")
    _, per, rows, cols = grad_ref.shape
    early = out_ref.shape[1]
    side = n * rows
    chunk = min(cols, 512)
    dests = partners(me, n)
    mine = pl.ds(pl.multiple_of(me * rows, rows), rows)

    def loads(c):
        slot = c % 2
        return (
            pltpu.make_async_copy(grad_ref.at[:, c], gs.at[slot], gload.at[slot]),
            pltpu.make_async_copy(mom_ref.at[:, c], ms.at[slot], mload.at[slot]),
        )

    def weight_load(c):
        slot = c % 2
        return pltpu.make_async_copy(weight_ref.at[:, c], ws.at[slot], wload.at[slot])

    def load(c):
        for copy in loads(c):
            copy.start()

    def make(c):
        for copy in loads(c):
            copy.wait()
        slot = c % 2

        def one(j, carry):
            new_ref[j, c] = hold_rate * ms[slot, j] + gs[slot, j]
            return carry

        lax.fori_loop(0, n, one, 0)

    def arrived(c, blocks, semaphore):
        got = out_ref.at[pl.ds(0, blocks), c]
        pltpu.make_async_copy(got, got, semaphore).wait()

    def finish(c):
        weight_load(c).wait()
        slot = c % 2

        def one(j, carry):
            out_ref[j, c] = (1.0 - learn_rate * decay_rate) * ws[slot, j] - learn_rate * out_ref[j, c]
            return carry

        lax.fori_loop(0, n, one, 0)

    def quarter_loads(k, quarter):
        at = pl.ds(quarter * part, part)
        return (
            pltpu.make_async_copy(grad_ref.at[at, 0], gs.at[0, at], qload.at[0, k]),
            pltpu.make_async_copy(mom_ref.at[at, 0], ms.at[0, at], qload.at[1, k]),
        )

    def quarter_make(k, quarter):
        for copy in quarter_loads(k, quarter):
            copy.wait()

        def one(j, carry):
            at = quarter * part + j
            new_ref[at, 0] = hold_rate * ms[0, at] + gs[0, at]
            return carry

        lax.fori_loop(0, part, one, 0)

    def forth(c):
        forth_to(c, dests)
        forth_own(c)

    def forth_own(c):
        pltpu.make_async_copy(new_ref.at[me, c], x.at[c, mine, :], recv1.at[c]).start()

    def forth_to(c, dests):
        for dest in dests:
            pltpu.make_async_remote_copy(
                src_ref=new_ref.at[dest, c],
                dst_ref=x.at[c, mine, :],
                send_sem=send1.at[c],
                recv_sem=recv1.at[c],
                device_id={"shard": dest},
                device_id_type=MESH,
            ).start()

    def back_own(c):
        pltpu.make_async_copy(x.at[c, mine, :], out_ref.at[me, c], recv2.at[c]).start()

    def back_to(c, dests, left, landed):
        for dest in dests:
            theirs = pl.ds(pl.multiple_of(dest * rows, rows), rows)
            pltpu.make_async_remote_copy(
                src_ref=x.at[c, theirs, :],
                dst_ref=out_ref.at[me, c],
                send_sem=left,
                recv_sem=landed,
                device_id={"shard": dest},
                device_id_type=MESH,
            ).start()

    part = n // 4
    own, beside, near, far = quarters(me, n)
    middle = (own == 1) | (own == 2)
    lead = jnp.where(middle, near, beside)
    third = jnp.where(middle, beside, near)
    firsts = (lead, own, third, far)

    barrier, count = greet(me, n, middle)
    for step in range(1, models):
        pl.semaphore_signal(barrier, inc=1, device_id={"model": (col + step) % models}, device_id_type=MESH)
    for k, quarter in enumerate(firsts):
        for copy in quarter_loads(k, quarter):
            copy.start()
    pl.semaphore_wait(barrier, count + models - 1)
    enter(me, n, middle, inside)
    quarter_make(0, lead)
    forth_to(0, members(me, n, lead))
    load(1)

    pass_across(me, n, middle, inside, passed)
    quarter_make(1, own)
    forth_to(0, members(me, n, own)[1:])
    forth_own(0)
    pass_outward(me, n, middle, passed)
    quarter_make(2, third)
    quarter_make(3, far)
    forth_to(0, woven(members(me, n, far), members(me, n, third)))
    for c in range(min(2, per)):
        weight_load(c).start()
    for c in range(2, min(AHEAD + 2, per + 1)):
        if c < per:
            load(c)
        make(c - 1)
    for c in range(1, min(AHEAD, per)):
        forth(c)

    eye = (
        lax.broadcasted_iota(jnp.int32, (side, side), 0) == lax.broadcasted_iota(jnp.int32, (side, side), 1)
    ).astype(jnp.float32)

    def round_(c, carry):
        pltpu.make_async_copy(x.at[c], x.at[c], recv1.at[c]).wait()

        def part(k, total):
            piece = x[c, :, pl.ds(pl.multiple_of(k * chunk, chunk), chunk)]
            return total + dot(piece, piece, ((1,), (1,)))

        gram[c] = lax.fori_loop(0, cols // chunk, part, jnp.zeros((side, side), jnp.float32))

        @pl.when(c + AHEAD < per)
        def _():
            forth(c + AHEAD)

        copies = []
        for step in range(1, models):
            copy = pltpu.make_async_remote_copy(
                src_ref=gram.at[c],
                dst_ref=peers.at[step - 1, c],
                send_sem=gsend.at[step - 1, c],
                recv_sem=grecv.at[step - 1, c],
                device_id={"model": (col + step) % models},
                device_id_type=MESH,
            )
            copy.start()
            copies.append(copy)
        whole = gram[c]
        for step, copy in enumerate(copies):
            copy.wait()
            whole = whole + peers[step, c]
        q = mixer(whole, eye)

        def apply(k, carry):
            at = pl.ds(pl.multiple_of(k * chunk, chunk), chunk)
            x[c, :, at] = mul(q, x[c, :, at])
            return carry

        lax.fori_loop(0, cols // chunk, apply, 0)

        @pl.when(c + AHEAD + 1 < per)
        def _():
            make(c + AHEAD + 1)

        @pl.when(c + AHEAD + 2 < per)
        def _():
            load(c + AHEAD + 2)

        holding = jnp.logical_and(jnp.logical_not(middle), c >= early - HELD)

        final = jnp.logical_and(middle, c == early - 1)

        @pl.when(jnp.logical_and(c < early - 1, jnp.logical_not(holding)))
        def _():
            back_to(c, dests, send2.at[c], recv2.at[c])

        @pl.when(final)
        def _():
            across = members(me, n, near) + members(me, n, far)
            others = woven(across, members(me, n, beside) + members(me, n, own)[1:])
            back_to(c, others, send2.at[c], recv2.at[c])

        @pl.when(jnp.logical_and(c < early, holding))
        def _():
            others = woven(members(me, n, beside), members(me, n, own)[1:]) + members(me, n, near)
            back_to(c, others, send2.at[c], recv2.at[c])

        @pl.when(c < early)
        def _():
            back_own(c)

        return carry

    lax.fori_loop(0, per, round_, 0)

    def drain(c, carry):
        sent = x.at[c, pl.ds(0, side - rows), :]
        pltpu.make_async_copy(sent, sent, send1.at[c]).wait()
        return carry

    lax.fori_loop(0, per, drain, 0)

    def last(c, carry):
        arrived(c, n, recv2.at[c])
        finish(c)

        @pl.when(c + 2 < early)
        def _():
            weight_load(c + 2).start()

        return carry

    lax.fori_loop(0, early - HELD, last, 0)

    outer = jnp.logical_not(middle)
    ends = tuple(enumerate(range(early - HELD, early)))

    def drained(c, blocks, semaphore):
        sent = x.at[c, pl.ds(0, blocks * rows), :]
        pltpu.make_async_copy(sent, sent, semaphore).wait()

    @pl.when(middle)
    def _():
        for _, c in ends:
            arrived(c, n, recv2.at[c])

    @pl.when(outer)
    def _():
        for _, c in ends:
            arrived(c, n - part, recv2.at[c])
        for k, c in ends:
            back_to(c, members(me, n, far), hsend.at[k], hrecv.at[k])
        for k, c in ends:
            arrived(c, part, hrecv.at[k])

    for _, c in ends:
        finish(c)

    def drain_back(c, carry):
        drained(c, n - 1, send2.at[c])
        return carry

    lax.fori_loop(0, early - HELD, drain_back, 0)

    @pl.when(middle)
    def _():
        for _, c in ends:
            drained(c, n - 1, send2.at[c])

    @pl.when(outer)
    def _():
        for k, c in ends:
            drained(c, n - 1 - part, send2.at[c])
            drained(c, part, hsend.at[k])


def tail_kernel(
    n, per, x, weight_ref, token_ref, out_ref, wlast_ref, ws, wload, send, recv, inside, passed,
):
    me = lax.axis_index("shard")
    _, late, rows, cols = out_ref.shape
    early = per - late
    own, beside, near, far = quarters(me, n)
    middle = (own == 1) | (own == 2)
    lead = jnp.where(middle, near, beside)
    third = jnp.where(middle, beside, near)

    def held(c):
        return wlast_ref if c == late - 1 else ws.at[c]

    def weight_load(c):
        return pltpu.make_async_copy(weight_ref.at[:, early + c], held(c), wload.at[c])

    def back_to(c, dests):
        for dest in dests:
            pltpu.make_async_remote_copy(
                src_ref=x.at[early + c, pl.ds(pl.multiple_of(dest * rows, rows), rows), :],
                dst_ref=out_ref.at[me, c],
                send_sem=send.at[c],
                recv_sem=recv.at[c],
                device_id={"shard": dest},
                device_id_type=MESH,
            ).start()

    barrier, count = greet(me, n, middle)
    pl.semaphore_wait(barrier, count)
    enter(me, n, middle, inside)
    for c in range(late - 1):
        back_to(c, members(me, n, lead))
    pass_across(me, n, middle, inside, passed)
    pass_outward(me, n, middle, passed)
    for c in range(late):
        if c < late - 1:
            back_to(c, woven(members(me, n, far), members(me, n, third)) + members(me, n, own)[1:])
        else:
            back_to(c, partners(me, n))
        mine = x.at[early + c, pl.ds(pl.multiple_of(me * rows, rows), rows), :]
        pltpu.make_async_copy(mine, out_ref.at[me, c], recv.at[c]).start()
    for c in range(late):
        weight_load(c).start()

    for c in range(late):
        got = out_ref.at[:, c]
        pltpu.make_async_copy(got, got, recv.at[c]).wait()
        weight_load(c).wait()
        if c < late - 1:

            def one(j, carry, c=c):
                out_ref[j, c] = (1.0 - learn_rate * decay_rate) * ws[c, j] - learn_rate * out_ref[j, c]
                return carry

            lax.fori_loop(0, n, one, 0)
    for c in range(late):
        sent = x.at[early + c, pl.ds(0, (n - 1) * rows), :]
        pltpu.make_async_copy(sent, sent, send.at[c]).wait()


def write_kernel(out_ref, new_ref, weights_ref, momentum_ref, token_ref, sems):
    n, early, _, _ = out_ref.shape
    token_ref[...] = jnp.zeros_like(token_ref)
    pieces = 4
    copies = []
    for k in range(pieces):
        at = pl.ds(k * (n // pieces), n // pieces)
        copies.append((new_ref.at[at], momentum_ref.at[at]))
        copies.append((out_ref.at[at], weights_ref.at[at, pl.ds(0, early)]))
    copies = [pltpu.make_async_copy(src, dst, sems.at[k]) for k, (src, dst) in enumerate(copies)]
    for copy in copies:
        copy.start()
    for copy in copies:
        copy.wait()


def close_kernel(begun_ref, out_ref, wlast_ref, weights_ref, stage, sems):
    n, late, _, _ = out_ref.shape
    per = weights_ref.shape[1]
    early = per - late
    ready = pltpu.make_async_copy(
        out_ref.at[:, pl.ds(0, late - 1)], weights_ref.at[:, pl.ds(early, late - 1)], sems.at[0]
    )
    ready.start()

    def one(j, carry):
        stage[j] = (1.0 - learn_rate * decay_rate) * wlast_ref[j] - learn_rate * out_ref[j, late - 1]
        return carry

    lax.fori_loop(0, n, one, 0)
    end = pltpu.make_async_copy(stage, weights_ref.at[:, per - 1], sems.at[1])
    end.start()
    ready.wait()
    end.wait()


def kept(array):
    return pltpu.with_memory_space_constraint(array, pltpu.VMEM)


def step_direct(gradients, momentum, weights, n, models):
    mats, rows, cols = gradients.shape
    per, side = mats // n, n * rows
    early = per - LATE
    others = max(models - 1, 1)
    split = (n, per, rows, cols)
    slab = (n, rows, cols)
    vmem, hbm = pl.BlockSpec(memory_space=pltpu.VMEM), pl.BlockSpec(memory_space=pltpu.HBM)
    whole = jax.ShapeDtypeStruct(split, jnp.float32)
    weights = weights.reshape(split)
    out, new, x = pl.pallas_call(
        functools.partial(step_kernel, n, models),
        out_shape=(
            pltpu.VMEM((n, early, rows, cols), jnp.float32),
            pltpu.VMEM(split, jnp.float32),
            pltpu.VMEM((per, side, cols), jnp.float32),
        ),
        in_specs=[hbm] * 3,
        out_specs=[vmem] * 3,
        scratch_shapes=[
            pltpu.VMEM((2, *slab), jnp.float32),
            pltpu.VMEM((2, *slab), jnp.float32),
            pltpu.VMEM((2, *slab), jnp.float32),
            pltpu.VMEM((per, side, side), jnp.float32),
            pltpu.VMEM((others, per, side, side), jnp.float32),
            pltpu.SemaphoreType.DMA((2,)),
            pltpu.SemaphoreType.DMA((2,)),
            pltpu.SemaphoreType.DMA((2,)),
            pltpu.SemaphoreType.DMA((2, 4)),
            pltpu.SemaphoreType.DMA((per,)),
            pltpu.SemaphoreType.DMA((per,)),
            pltpu.SemaphoreType.DMA((early,)),
            pltpu.SemaphoreType.DMA((early,)),
            pltpu.SemaphoreType.DMA((HELD,)),
            pltpu.SemaphoreType.DMA((HELD,)),
            pltpu.SemaphoreType.DMA((others, per)),
            pltpu.SemaphoreType.DMA((others, per)),
            pltpu.SemaphoreType.REGULAR,
            pltpu.SemaphoreType.REGULAR,
        ],
        compiler_params=pltpu.CompilerParams(
            collective_id=0, has_side_effects=True, vmem_limit_bytes=40 * 1024 * 1024
        ),
    )(gradients.reshape(split), momentum.reshape(split), weights)
    begun, new, token = pl.pallas_call(
        write_kernel,
        out_shape=(whole, whole, pltpu.VMEM((8, 128), jnp.float32)),
        in_specs=[vmem] * 2,
        out_specs=[hbm, hbm, vmem],
        scratch_shapes=[pltpu.SemaphoreType.DMA((8,))],
        compiler_params=pltpu.CompilerParams(vmem_limit_bytes=4 * 1024 * 1024),
    )(kept(out), kept(new))
    out, wlast = pl.pallas_call(
        functools.partial(tail_kernel, n, per),
        out_shape=(pltpu.VMEM((n, LATE, rows, cols), jnp.float32), pltpu.VMEM(slab, jnp.float32)),
        in_specs=[vmem, hbm, vmem],
        out_specs=[vmem] * 2,
        scratch_shapes=[
            pltpu.VMEM((LATE - 1, *slab), jnp.float32),
            pltpu.SemaphoreType.DMA((LATE,)),
            pltpu.SemaphoreType.DMA((LATE,)),
            pltpu.SemaphoreType.DMA((LATE,)),
            pltpu.SemaphoreType.REGULAR,
            pltpu.SemaphoreType.REGULAR,
        ],
        compiler_params=pltpu.CompilerParams(
            collective_id=1, has_side_effects=True, vmem_limit_bytes=38 * 1024 * 1024
        ),
    )(kept(x), weights, kept(token))
    done = pl.pallas_call(
        close_kernel,
        out_shape=whole,
        in_specs=[hbm, vmem, vmem],
        out_specs=hbm,
        scratch_shapes=[pltpu.VMEM(slab, jnp.float32), pltpu.SemaphoreType.DMA((2,))],
        input_output_aliases={0: 0},
        compiler_params=pltpu.CompilerParams(vmem_limit_bytes=4 * 1024 * 1024),
    )(begun, kept(out), kept(wlast))
    return done.reshape(gradients.shape), new.reshape(gradients.shape)


def exchange_plain(new_momentum):
    moved = lax.all_to_all(new_momentum, "shard", split_axis=0, concat_axis=1, tiled=True)
    gram = lax.psum(
        jnp.einsum("mik,mjk->mij", moved, moved, precision=lax.Precision.HIGHEST), "model"
    )
    eye = jnp.eye(gram.shape[-1], dtype=jnp.float32)
    q = jax.vmap(lambda g: mixer(g, eye))(gram)
    iterate = jnp.einsum("mij,mjk->mik", q, moved, precision=lax.Precision.HIGHEST)
    return lax.all_to_all(iterate, "shard", split_axis=1, concat_axis=0, tiled=True)


def body(n, models, gradients, momentum, weights):
    mats, rows, cols = gradients.shape
    size = mats * rows * cols * 4
    if n & (n - 1) == 0 and rows % 8 == 0 and cols % 128 == 0 and size <= 8 << 20 and mats // n > LATE + HELD and n % 4 == 0:
        return step_direct(gradients, momentum, weights, n, models)
    new_momentum = hold_rate * momentum + gradients
    back = exchange_plain(new_momentum)
    new_weights = (1.0 - learn_rate * decay_rate) * weights - learn_rate * back
    return (new_weights, new_momentum)


def solution(mesh):
    placed = (P(None, "shard", "model"), P(None, "shard", "model"), P(None, "shard", "model"))
    return jax.shard_map(
        functools.partial(body, mesh.shape["shard"], mesh.shape["model"]),
        mesh=mesh,
        in_specs=placed,
        out_specs=(P(None, "shard", "model"), P(None, "shard", "model")),
        check_vma=False,
    )
```

```python
import functools

import jax
import jax.numpy as jnp
from jax import lax
from jax.experimental import pallas as pl
from jax.experimental.pallas import tpu as pltpu
from jax.sharding import PartitionSpec as P

ITERS = 3
AHEAD = 7
LATE = 3
HELD = 1

hold_rate = 0.9
learn_rate = 0.9
decay_rate = 0.1

MESH = pl.DeviceIdType.MESH


def dot(a, b, contract):
    return lax.dot_general(
        a,
        b,
        ((contract[0], contract[1]), ((), ())),
        precision=lax.Precision.HIGHEST,
        preferred_element_type=jnp.float32,
    )


def mul(a, b):
    return dot(a, b, ((1,), (0,)))


def mixer(gram, eye):
    total = jnp.sum(jnp.sum(gram * eye, axis=1, keepdims=True), axis=0, keepdims=True)
    scale = lax.rsqrt(total + 1e-06)
    a = gram * scale * scale
    q = None
    for step in range(ITERS):
        p = 3.4445 * eye + (-4.775 * a + 2.0315 * mul(a, a))
        q = p if q is None else mul(p, q)
        if step < ITERS - 1:
            a = mul(mul(p, a), p)
    return q * scale


def flipped(me, k, n):
    out, bit = 0, 1
    while bit < n:
        own = (me // bit) % 2
        out = out + bit * ((1 - own) if (k // bit) % 2 else own)
        bit *= 2
    return out


def quarters(me, n):
    at = me // (n // 4)
    upper = at // 2
    return at, at + 1 - 2 * (at % 2), 2 - upper, 3 * (1 - upper)


def members(me, n, quarter):
    part = n // 4
    return [part * quarter + flipped(me % part, k, part) for k in range(part)]


def woven(first, second):
    order = []
    for k in range(max(len(first), len(second))):
        order += first[k : k + 1] + second[k : k + 1]
    return order


def partners(me, n):
    own, beside, near, far = (members(me, n, quarter) for quarter in quarters(me, n))
    return woven(far + near, beside + own[1:])


def signal(semaphore, dest):
    pl.semaphore_signal(semaphore, inc=1, device_id={"shard": dest}, device_id_type=MESH)


def greet(me, n, middle):
    _, beside, near, _ = quarters(me, n)
    barrier = pltpu.get_barrier_semaphore()

    @pl.when(middle)
    def _():
        for dest in members(me, n, near) + members(me, n, beside):
            signal(barrier, dest)

    own = members(me, n, quarters(me, n)[0])
    for dest in own[1:]:
        signal(barrier, dest)
    return barrier, len(own) * 2 - 1


def enter(me, n, middle, inside):
    @pl.when(jnp.logical_not(middle))
    def _():
        for dest in members(me, n, quarters(me, n)[1]):
            signal(inside, dest)


def pass_across(me, n, middle, inside, passed):
    @pl.when(middle)
    def _():
        pl.semaphore_wait(inside, n // 4)
        signal(passed, members(me, n, quarters(me, n)[2])[0])


def pass_outward(me, n, middle, passed):
    pl.semaphore_wait(passed, 1)

    @pl.when(middle)
    def _():
        signal(passed, members(me, n, quarters(me, n)[1])[0])


def step_kernel(
    n, models, grad_ref, mom_ref, weight_ref, out_ref, new_ref, x,
    gs, ms, ws, gram, peers, gload, mload, wload, qload, send1, recv1, send2, recv2, hsend, hrecv, gsend, grecv, inside, passed,
):
    me = lax.axis_index("shard")
    col = lax.axis_index("model")
    _, per, rows, cols = grad_ref.shape
    early = out_ref.shape[1]
    side = n * rows
    chunk = min(cols, 512)
    dests = partners(me, n)
    mine = pl.ds(pl.multiple_of(me * rows, rows), rows)

    def loads(c):
        slot = c % 2
        return (
            pltpu.make_async_copy(grad_ref.at[:, c], gs.at[slot], gload.at[slot]),
            pltpu.make_async_copy(mom_ref.at[:, c], ms.at[slot], mload.at[slot]),
        )

    def weight_load(c):
        slot = c % 2
        return pltpu.make_async_copy(weight_ref.at[:, c], ws.at[slot], wload.at[slot])

    def load(c):
        for copy in loads(c):
            copy.start()

    def make(c):
        for copy in loads(c):
            copy.wait()
        slot = c % 2

        def one(j, carry):
            new_ref[j, c] = hold_rate * ms[slot, j] + gs[slot, j]
            return carry

        lax.fori_loop(0, n, one, 0)

    def arrived(c, blocks, semaphore):
        got = out_ref.at[pl.ds(0, blocks), c]
        pltpu.make_async_copy(got, got, semaphore).wait()

    def finish(c):
        weight_load(c).wait()
        slot = c % 2

        def one(j, carry):
            out_ref[j, c] = (1.0 - learn_rate * decay_rate) * ws[slot, j] - learn_rate * out_ref[j, c]
            return carry

        lax.fori_loop(0, n, one, 0)

    def quarter_loads(k, quarter):
        at = pl.ds(quarter * part, part)
        return (
            pltpu.make_async_copy(grad_ref.at[at, 0], gs.at[0, at], qload.at[0, k]),
            pltpu.make_async_copy(mom_ref.at[at, 0], ms.at[0, at], qload.at[1, k]),
        )

    def quarter_make(k, quarter):
        for copy in quarter_loads(k, quarter):
            copy.wait()

        def one(j, carry):
            at = quarter * part + j
            new_ref[at, 0] = hold_rate * ms[0, at] + gs[0, at]
            return carry

        lax.fori_loop(0, part, one, 0)

    def forth(c):
        forth_to(c, dests)
        forth_own(c)

    def forth_own(c):
        pltpu.make_async_copy(new_ref.at[me, c], x.at[c, mine, :], recv1.at[c]).start()

    def forth_to(c, dests):
        for dest in dests:
            pltpu.make_async_remote_copy(
                src_ref=new_ref.at[dest, c],
                dst_ref=x.at[c, mine, :],
                send_sem=send1.at[c],
                recv_sem=recv1.at[c],
                device_id={"shard": dest},
                device_id_type=MESH,
            ).start()

    def back_own(c):
        pltpu.make_async_copy(x.at[c, mine, :], out_ref.at[me, c], recv2.at[c]).start()

    def back_to(c, dests, left, landed):
        for dest in dests:
            theirs = pl.ds(pl.multiple_of(dest * rows, rows), rows)
            pltpu.make_async_remote_copy(
                src_ref=x.at[c, theirs, :],
                dst_ref=out_ref.at[me, c],
                send_sem=left,
                recv_sem=landed,
                device_id={"shard": dest},
                device_id_type=MESH,
            ).start()

    part = n // 4
    own, beside, near, far = quarters(me, n)
    middle = (own == 1) | (own == 2)
    lead = jnp.where(middle, near, beside)
    third = jnp.where(middle, beside, near)
    firsts = (lead, own, third, far)

    barrier, count = greet(me, n, middle)
    for step in range(1, models):
        pl.semaphore_signal(barrier, inc=1, device_id={"model": (col + step) % models}, device_id_type=MESH)
    for k, quarter in enumerate(firsts):
        for copy in quarter_loads(k, quarter):
            copy.start()
    pl.semaphore_wait(barrier, count + models - 1)
    enter(me, n, middle, inside)
    quarter_make(0, lead)
    forth_to(0, members(me, n, lead))
    load(1)

    pass_across(me, n, middle, inside, passed)
    quarter_make(1, own)
    forth_to(0, members(me, n, own)[1:])
    forth_own(0)
    pass_outward(me, n, middle, passed)
    quarter_make(2, third)
    quarter_make(3, far)
    forth_to(0, woven(members(me, n, far), members(me, n, third)))
    for c in range(min(2, per)):
        weight_load(c).start()
    for c in range(2, min(AHEAD + 2, per + 1)):
        if c < per:
            load(c)
        make(c - 1)
    for c in range(1, min(AHEAD, per)):
        forth(c)

    eye = (
        lax.broadcasted_iota(jnp.int32, (side, side), 0) == lax.broadcasted_iota(jnp.int32, (side, side), 1)
    ).astype(jnp.float32)

    def round_(c, carry):
        pltpu.make_async_copy(x.at[c], x.at[c], recv1.at[c]).wait()

        def part(k, total):
            piece = x[c, :, pl.ds(pl.multiple_of(k * chunk, chunk), chunk)]
            return total + dot(piece, piece, ((1,), (1,)))

        gram[c] = lax.fori_loop(0, cols // chunk, part, jnp.zeros((side, side), jnp.float32))

        @pl.when(c + AHEAD < per)
        def _():
            forth(c + AHEAD)

        copies = []
        for step in range(1, models):
            copy = pltpu.make_async_remote_copy(
                src_ref=gram.at[c],
                dst_ref=peers.at[step - 1, c],
                send_sem=gsend.at[step - 1, c],
                recv_sem=grecv.at[step - 1, c],
                device_id={"model": (col + step) % models},
                device_id_type=MESH,
            )
            copy.start()
            copies.append(copy)
        whole = gram[c]
        for step, copy in enumerate(copies):
            copy.wait()
            whole = whole + peers[step, c]
        q = mixer(whole, eye)

        def apply(k, carry):
            at = pl.ds(pl.multiple_of(k * chunk, chunk), chunk)
            x[c, :, at] = mul(q, x[c, :, at])
            return carry

        lax.fori_loop(0, cols // chunk, apply, 0)

        @pl.when(c + AHEAD + 1 < per)
        def _():
            make(c + AHEAD + 1)

        @pl.when(c + AHEAD + 2 < per)
        def _():
            load(c + AHEAD + 2)

        holding = jnp.logical_and(jnp.logical_not(middle), c >= early - HELD)

        final = jnp.logical_and(middle, c == early - 1)

        @pl.when(jnp.logical_and(c < early - 1, jnp.logical_not(holding)))
        def _():
            back_to(c, dests, send2.at[c], recv2.at[c])

        @pl.when(final)
        def _():
            across = members(me, n, near) + members(me, n, far)
            others = woven(across, members(me, n, beside) + members(me, n, own)[1:])
            back_to(c, others, send2.at[c], recv2.at[c])

        @pl.when(jnp.logical_and(c < early, holding))
        def _():
            others = woven(members(me, n, beside), members(me, n, own)[1:]) + members(me, n, near)
            back_to(c, others, send2.at[c], recv2.at[c])

        @pl.when(c < early)
        def _():
            back_own(c)

        return carry

    lax.fori_loop(0, per, round_, 0)

    def drain(c, carry):
        sent = x.at[c, pl.ds(0, side - rows), :]
        pltpu.make_async_copy(sent, sent, send1.at[c]).wait()
        return carry

    lax.fori_loop(0, per, drain, 0)

    def last(c, carry):
        arrived(c, n, recv2.at[c])
        finish(c)

        @pl.when(c + 2 < early)
        def _():
            weight_load(c + 2).start()

        return carry

    lax.fori_loop(0, early - HELD, last, 0)

    outer = jnp.logical_not(middle)
    ends = tuple(enumerate(range(early - HELD, early)))

    def drained(c, blocks, semaphore):
        sent = x.at[c, pl.ds(0, blocks * rows), :]
        pltpu.make_async_copy(sent, sent, semaphore).wait()

    @pl.when(middle)
    def _():
        for _, c in ends:
            arrived(c, n, recv2.at[c])

    @pl.when(outer)
    def _():
        for _, c in ends:
            arrived(c, n - part, recv2.at[c])
        for k, c in ends:
            back_to(c, members(me, n, far), hsend.at[k], hrecv.at[k])
        for k, c in ends:
            arrived(c, part, hrecv.at[k])

    for _, c in ends:
        finish(c)

    def drain_back(c, carry):
        drained(c, n - 1, send2.at[c])
        return carry

    lax.fori_loop(0, early - HELD, drain_back, 0)

    @pl.when(middle)
    def _():
        for _, c in ends:
            drained(c, n - 1, send2.at[c])

    @pl.when(outer)
    def _():
        for k, c in ends:
            drained(c, n - 1 - part, send2.at[c])
            drained(c, part, hsend.at[k])


def tail_kernel(
    n, per, x, weight_ref, token_ref, out_ref, wlast_ref, ws, wload, send, recv, inside, passed,
):
    me = lax.axis_index("shard")
    _, late, rows, cols = out_ref.shape
    early = per - late
    own, beside, near, far = quarters(me, n)
    middle = (own == 1) | (own == 2)
    lead = jnp.where(middle, near, beside)
    third = jnp.where(middle, beside, near)

    def held(c):
        return wlast_ref if c == late - 1 else ws.at[c]

    def weight_load(c):
        return pltpu.make_async_copy(weight_ref.at[:, early + c], held(c), wload.at[c])

    def back_to(c, dests):
        for dest in dests:
            pltpu.make_async_remote_copy(
                src_ref=x.at[early + c, pl.ds(pl.multiple_of(dest * rows, rows), rows), :],
                dst_ref=out_ref.at[me, c],
                send_sem=send.at[c],
                recv_sem=recv.at[c],
                device_id={"shard": dest},
                device_id_type=MESH,
            ).start()

    barrier, count = greet(me, n, middle)
    pl.semaphore_wait(barrier, count)
    enter(me, n, middle, inside)
    for c in range(late - 1):
        back_to(c, members(me, n, lead))
    pass_across(me, n, middle, inside, passed)
    pass_outward(me, n, middle, passed)
    for c in range(late):
        if c < late - 1:
            back_to(c, woven(members(me, n, far), members(me, n, third)) + members(me, n, own)[1:])
        else:
            back_to(c, partners(me, n))
        mine = x.at[early + c, pl.ds(pl.multiple_of(me * rows, rows), rows), :]
        pltpu.make_async_copy(mine, out_ref.at[me, c], recv.at[c]).start()
    for c in range(late):
        weight_load(c).start()

    for c in range(late):
        got = out_ref.at[:, c]
        pltpu.make_async_copy(got, got, recv.at[c]).wait()
        weight_load(c).wait()
        if c < late - 1:

            def one(j, carry, c=c):
                out_ref[j, c] = (1.0 - learn_rate * decay_rate) * ws[c, j] - learn_rate * out_ref[j, c]
                return carry

            lax.fori_loop(0, n, one, 0)
    for c in range(late):
        sent = x.at[early + c, pl.ds(0, (n - 1) * rows), :]
        pltpu.make_async_copy(sent, sent, send.at[c]).wait()


def write_kernel(out_ref, new_ref, weights_ref, momentum_ref, token_ref, sems):
    n, early, _, _ = out_ref.shape
    token_ref[...] = jnp.zeros_like(token_ref)
    pieces = 4
    copies = []
    for k in range(pieces):
        at = pl.ds(k * (n // pieces), n // pieces)
        copies.append((new_ref.at[at], momentum_ref.at[at]))
        copies.append((out_ref.at[at], weights_ref.at[at, pl.ds(0, early)]))
    copies = [pltpu.make_async_copy(src, dst, sems.at[k]) for k, (src, dst) in enumerate(copies)]
    for copy in copies:
        copy.start()
    for copy in copies:
        copy.wait()


def close_kernel(begun_ref, out_ref, wlast_ref, weights_ref, stage, sems):
    n, late, _, _ = out_ref.shape
    per = weights_ref.shape[1]
    early = per - late
    ready = pltpu.make_async_copy(
        out_ref.at[:, pl.ds(0, late - 1)], weights_ref.at[:, pl.ds(early, late - 1)], sems.at[0]
    )
    ready.start()

    def one(j, carry):
        stage[j] = (1.0 - learn_rate * decay_rate) * wlast_ref[j] - learn_rate * out_ref[j, late - 1]
        return carry

    lax.fori_loop(0, n, one, 0)
    end = pltpu.make_async_copy(stage, weights_ref.at[:, per - 1], sems.at[1])
    end.start()
    ready.wait()
    end.wait()


def kept(array):
    return pltpu.with_memory_space_constraint(array, pltpu.VMEM)


def step_direct(gradients, momentum, weights, n, models):
    mats, rows, cols = gradients.shape
    per, side = mats // n, n * rows
    early = per - LATE
    others = max(models - 1, 1)
    split = (n, per, rows, cols)
    slab = (n, rows, cols)
    vmem, hbm = pl.BlockSpec(memory_space=pltpu.VMEM), pl.BlockSpec(memory_space=pltpu.HBM)
    whole = jax.ShapeDtypeStruct(split, jnp.float32)
    weights = weights.reshape(split)
    out, new, x = pl.pallas_call(
        functools.partial(step_kernel, n, models),
        out_shape=(
            pltpu.VMEM((n, early, rows, cols), jnp.float32),
            pltpu.VMEM(split, jnp.float32),
            pltpu.VMEM((per, side, cols), jnp.float32),
        ),
        in_specs=[hbm] * 3,
        out_specs=[vmem] * 3,
        scratch_shapes=[
            pltpu.VMEM((2, *slab), jnp.float32),
            pltpu.VMEM((2, *slab), jnp.float32),
            pltpu.VMEM((2, *slab), jnp.float32),
            pltpu.VMEM((per, side, side), jnp.float32),
            pltpu.VMEM((others, per, side, side), jnp.float32),
            pltpu.SemaphoreType.DMA((2,)),
            pltpu.SemaphoreType.DMA((2,)),
            pltpu.SemaphoreType.DMA((2,)),
            pltpu.SemaphoreType.DMA((2, 4)),
            pltpu.SemaphoreType.DMA((per,)),
            pltpu.SemaphoreType.DMA((per,)),
            pltpu.SemaphoreType.DMA((early,)),
            pltpu.SemaphoreType.DMA((early,)),
            pltpu.SemaphoreType.DMA((HELD,)),
            pltpu.SemaphoreType.DMA((HELD,)),
            pltpu.SemaphoreType.DMA((others, per)),
            pltpu.SemaphoreType.DMA((others, per)),
            pltpu.SemaphoreType.REGULAR,
            pltpu.SemaphoreType.REGULAR,
        ],
        compiler_params=pltpu.CompilerParams(
            collective_id=0, has_side_effects=True, vmem_limit_bytes=40 * 1024 * 1024
        ),
    )(gradients.reshape(split), momentum.reshape(split), weights)
    begun, new, token = pl.pallas_call(
        write_kernel,
        out_shape=(whole, whole, pltpu.VMEM((8, 128), jnp.float32)),
        in_specs=[vmem] * 2,
        out_specs=[hbm, hbm, vmem],
        scratch_shapes=[pltpu.SemaphoreType.DMA((8,))],
        compiler_params=pltpu.CompilerParams(vmem_limit_bytes=4 * 1024 * 1024),
    )(kept(out), kept(new))
    out, wlast = pl.pallas_call(
        functools.partial(tail_kernel, n, per),
        out_shape=(pltpu.VMEM((n, LATE, rows, cols), jnp.float32), pltpu.VMEM(slab, jnp.float32)),
        in_specs=[vmem, hbm, vmem],
        out_specs=[vmem] * 2,
        scratch_shapes=[
            pltpu.VMEM((LATE - 1, *slab), jnp.float32),
            pltpu.SemaphoreType.DMA((LATE,)),
            pltpu.SemaphoreType.DMA((LATE,)),
            pltpu.SemaphoreType.DMA((LATE,)),
            pltpu.SemaphoreType.REGULAR,
            pltpu.SemaphoreType.REGULAR,
        ],
        compiler_params=pltpu.CompilerParams(
            collective_id=1, has_side_effects=True, vmem_limit_bytes=38 * 1024 * 1024
        ),
    )(kept(x), weights, kept(token))
    done = pl.pallas_call(
        close_kernel,
        out_shape=whole,
        in_specs=[hbm, vmem, vmem],
        out_specs=hbm,
        scratch_shapes=[pltpu.VMEM(slab, jnp.float32), pltpu.SemaphoreType.DMA((2,))],
        input_output_aliases={0: 0},
        compiler_params=pltpu.CompilerParams(vmem_limit_bytes=4 * 1024 * 1024),
    )(begun, kept(out), kept(wlast))
    return done.reshape(gradients.shape), new.reshape(gradients.shape)


def exchange_plain(new_momentum):
    moved = lax.all_to_all(new_momentum, "shard", split_axis=0, concat_axis=1, tiled=True)
    gram = lax.psum(
        jnp.einsum("mik,mjk->mij", moved, moved, precision=lax.Precision.HIGHEST), "model"
    )
    eye = jnp.eye(gram.shape[-1], dtype=jnp.float32)
    q = jax.vmap(lambda g: mixer(g, eye))(gram)
    iterate = jnp.einsum("mij,mjk->mik", q, moved, precision=lax.Precision.HIGHEST)
    return lax.all_to_all(iterate, "shard", split_axis=1, concat_axis=0, tiled=True)


def body(n, models, gradients, momentum, weights):
    mats, rows, cols = gradients.shape
    size = mats * rows * cols * 4
    if n & (n - 1) == 0 and rows % 8 == 0 and cols % 128 == 0 and size <= 8 << 20 and mats // n > LATE + HELD and n % 4 == 0:
        return step_direct(gradients, momentum, weights, n, models)
    new_momentum = hold_rate * momentum + gradients
    back = exchange_plain(new_momentum)
    new_weights = (1.0 - learn_rate * decay_rate) * weights - learn_rate * back
    return (new_weights, new_momentum)


def solution(mesh):
    placed = (P(None, "shard", "model"), P(None, "shard", "model"), P(None, "shard", "model"))
    return jax.shard_map(
        functools.partial(body, mesh.shape["shard"], mesh.shape["model"]),
        mesh=mesh,
        in_specs=placed,
        out_specs=(P(None, "shard", "model"), P(None, "shard", "model")),
        check_vma=False,
    )
```
